512 devices in a mesh: share: 16 (over z, core), row: 32 (over y, x).
Axes of the slice: x: 4, y: 8, z: 8, core: 2. Of those that a mesh axis runs over, the one named last changes fastest.
Arguments:
- remaining_coded_pieces: float32 [16, 512, 8192], P('share', 'row'), may hold values from -6 to 6
- alive_piece_indices: int32 [16], replicated, may hold values from 0 to 19, as said below
- slab_starting_positions: int32 [2], replicated, may hold values from 0 to 48
Outputs:
- decoded: float32 [16, 512, 4096], P('share', None, 'row')
The draws below stay inside these ranges and needn't reach their ends.
Inputs may be any that keep to these rules, and one draw needn't show every extreme that they name: `alive_piece_indices`: 16 different share numbers in rising order.
All inputs are finite; a program needn't handle non-finite values.
Results may differ from the reference program's by a relative error of at most 0.00007.
Values sent between devices are 32-bit elements; how exact they have to be, the bound alone decides.
A program may use at most 64 MiB of HBM per device.

```python
import jax
import jax.numpy as jnp
from jax import lax

K = 16
CODED_PIECES_ALL = 20
W = 2048
COLS = 8192
R_WIN = 512


def draw_alive_piece_indices(key, part):
    shuffled = jax.random.permutation(jax.random.fold_in(key, 7), CODED_PIECES_ALL)
    return jnp.sort(shuffled[:K]).astype(jnp.int32)


def block_scale(stream_key, dims, split, least, top_value):
    def one(dim, blocks):
        draws = jax.random.uniform(jax.random.fold_in(jax.random.fold_in(stream_key, 6), dim), (blocks,), jnp.float32, least / len(split), top_value / len(split))
        return jnp.repeat(jnp.exp(draws), dims[dim] // blocks).reshape((-1,) + (1,) * (len(dims) - dim - 1))

    level = one(*split[0])
    for cut in split[1:]:
        level = level * one(*cut)
    return level


def noise(stream_key, extent, deviation, limit, cuts=(), held_as=jnp.bfloat16):
    level = block_scale(stream_key, extent, cuts, -0.22, 0.18) if cuts else 1.0
    values = jax.random.normal(stream_key, extent, jnp.float32) * deviation * level
    return jnp.minimum(jnp.maximum(values, -limit), limit).astype(held_as)


def setup_inputs(seed: int = 0) -> dict:
    keys = jax.random.split(jax.random.key(seed), 4)
    remaining_coded_pieces = noise(keys[0], (K, R_WIN, COLS), 1.0, 6.0, ((0, 16), (1, 32)), jnp.float32)
    alive_piece_indices = draw_alive_piece_indices(jax.random.fold_in(keys[3], 71), 0)
    slab_starting_positions = jax.random.randint(keys[2], (2,), 0, (COLS - W) // 128 + 1).astype(jnp.int32)
    return dict(remaining_coded_pieces=remaining_coded_pieces, alive_piece_indices=alive_piece_indices, slab_starting_positions=slab_starting_positions)


def recovery_operator(alive_piece_indices):
    numbers = jnp.arange(CODED_PIECES_ALL, dtype=jnp.float32)
    nodes = jnp.cos(jnp.pi * (2.0 * numbers + 1.0) / (2.0 * CODED_PIECES_ALL))
    chosen_coded_pieces = (alive_piece_indices[:, None] == jnp.arange(CODED_PIECES_ALL, dtype=jnp.int32)[None, :]).astype(jnp.float32)
    points = jnp.sum(chosen_coded_pieces * nodes[None, :], axis=1)
    polynomial_degrees = jnp.arange(K, dtype=jnp.float32)
    angles = jnp.pi * (2.0 * polynomial_degrees + 1.0) / (2.0 * K)
    samples = jnp.cos(angles)
    same = jnp.arange(K, dtype=jnp.int32)[:, None] == jnp.arange(K, dtype=jnp.int32)[None, :]
    spacing = jnp.where(same, 1.0, points[:, None] - points[None, :])
    factors = (samples[None, None, :] - points[None, :, None]) / spacing[:, :, None]
    factors = jnp.where(same[:, :, None], 1.0, factors)
    lagrange = jnp.prod(factors, axis=1)
    table = jnp.cos(polynomial_degrees[:, None] * angles[None, :])
    recovery_coefficients = (2.0 / K) * jnp.sum(table[:, None, :] * lagrange[None, :, :], axis=2)
    return recovery_coefficients * jnp.where(polynomial_degrees == 0.0, 0.5, 1.0)[:, None]


def reference(remaining_coded_pieces, alive_piece_indices, slab_starting_positions):
    recovery_coefficients = recovery_operator(alive_piece_indices)
    first = lax.dynamic_slice_in_dim(remaining_coded_pieces, (slab_starting_positions[0] * 128).astype(jnp.int32), W, 2)
    second = lax.dynamic_slice_in_dim(remaining_coded_pieces, (slab_starting_positions[1] * 128).astype(jnp.int32), W, 2)
    slabs = jnp.concatenate([first, second], axis=2)
    return jnp.einsum("ki,irc->krc", recovery_coefficients, slabs, precision=lax.Precision.HIGHEST)
```

```python
import functools

import jax
import jax.numpy as jnp
import numpy as np
from jax import lax
from jax.experimental import pallas as pl
from jax.experimental.pallas import tpu as pltpu
from jax.sharding import PartitionSpec as P

K = 16
CODED_PIECES_ALL = 20
W = 2048
LANES = 128
SUBLANES = 8
CHUNKS = 1
MESH = pl.DeviceIdType.MESH


def constants():
    table = np.zeros((24, LANES), np.float32)
    theta = np.pi * (2.0 * np.arange(K) + 1.0) / (2.0 * K)
    degrees = np.arange(K)[:, None]
    scale = np.where(degrees == 0, 1.0, 2.0) / K
    table[:K, :K] = scale * np.cos(degrees * theta[None, :])
    table[K, :K] = np.cos(theta)
    numbers = np.arange(CODED_PIECES_ALL)
    table[K + 1, :CODED_PIECES_ALL] = np.cos(np.pi * (2.0 * numbers + 1.0) / (2.0 * CODED_PIECES_ALL))
    return table


def weights_into(table, alive, points_ref, w_ref):
    rows = lax.broadcasted_iota(jnp.int32, (K, LANES), 0)
    lanes = lax.broadcasted_iota(jnp.int32, (K, LANES), 1)
    number = jnp.zeros((K, LANES), jnp.int32)
    for i in range(K):
        number = jnp.where(rows == i, alive[i], number)
    nodes = jnp.broadcast_to(table[K + 1 : K + 2, :], (K, LANES))
    points = jnp.sum(jnp.where(lanes == number, nodes, 0.0), axis=1, keepdims=True)
    points = jnp.broadcast_to(points, (K, LANES))
    points_ref[...] = points
    samples = table[K : K + 1, :]
    over = jnp.ones((K, LANES), jnp.float32)
    under = jnp.ones((K, LANES), jnp.float32)
    for j in range(K):
        point = points_ref[j : j + 1, :]
        over = over * jnp.where(rows == j, 1.0, samples - point)
        under = under * jnp.where(rows == j, 1.0, points - point)
    lagrange = over / under
    for k in range(K):
        total = jnp.sum(lagrange * table[k : k + 1, :], axis=1, keepdims=True)
        w_ref[k] = jnp.broadcast_to(total, (K, LANES))


def kernel(
    shares, rows, chunks,
    alive, starts, x_hbm, table_hbm, out,
    x, table, points, w, send_a, got_a, got_b, send_c,
    load_sems, a_send, a_recv, b_send, b_recv, c_send, c_recv,
):
    me_s = lax.axis_index("share")
    me_r = lax.axis_index("row")
    load_x = pltpu.make_async_copy(x_hbm, x, load_sems.at[0])
    load_t = pltpu.make_async_copy(table_hbm, table, load_sems.at[1])
    load_x.start()
    load_t.start()

    barrier = pltpu.get_barrier_semaphore()
    for d in range(1, rows):
        pl.semaphore_signal(barrier, inc=1, device_id=(me_s, lax.rem(me_r + d, rows)), device_id_type=MESH)
    for d in range(1, shares):
        pl.semaphore_signal(barrier, inc=1, device_id=(lax.rem(me_s + d, shares), me_r), device_id_type=MESH)

    tiles = x.shape[0] // chunks
    step = tiles * SUBLANES
    load_x.wait()
    for h in range(2):
        first = starts[h]
        for c in range(chunks):
            for t in range(tiles):
                for b in range(W // LANES):
                    block = x[c * tiles + t, first + b]
                    send_a[c, h * (W // LANES) + b, t * SUBLANES : (t + 1) * SUBLANES] = block
    pl.semaphore_wait(barrier, rows - 1 + shares - 1)

    for c in range(chunks):
        for d in range(1, rows):
            to = lax.rem(me_r + d, rows)
            pltpu.make_async_remote_copy(
                src_ref=send_a.at[c, to], dst_ref=got_a.at[c, me_r],
                send_sem=a_send, recv_sem=a_recv.at[c], device_id=(me_s, to), device_id_type=MESH,
            ).start()
    for c in range(chunks):
        got_a[c, me_r] = send_a[c, me_r]

    load_t.wait()
    weights_into(table, alive, points, w)

    def waits(ref, send, recv):
        return pltpu.make_async_remote_copy(
            src_ref=ref, dst_ref=ref, send_sem=send, recv_sem=recv, device_id=(me_s, me_r), device_id_type=MESH
        )

    for c in range(chunks):
        waits(got_a.at[c, pl.ds(0, rows - 1)], a_send, a_recv.at[c]).wait_recv()
        for d in range(1, shares):
            to = lax.rem(me_s + d, shares)
            pltpu.make_async_remote_copy(
                src_ref=got_a.at[c, pl.ds(2 * to, 2)], dst_ref=got_b.at[c, me_s],
                send_sem=b_send, recv_sem=b_recv.at[c], device_id=(to, me_r), device_id_type=MESH,
            ).start()
        got_b[c, me_s] = got_a[c, pl.ds(2 * me_s, 2)]

    for c in range(chunks):
        waits(got_b.at[c, pl.ds(0, shares - 1)], b_send, b_recv.at[c]).wait_recv()
        for h in range(2):
            data = [got_b[c, i, h] for i in range(K)]
            for k in range(K):
                total = w[k, 0:1, :] * data[0]
                for i in range(1, K):
                    total = total + w[k, i : i + 1, :] * data[i]
                send_c[c, k, h] = total
        for d in range(1, shares):
            to = lax.rem(me_s + d, shares)
            pltpu.make_async_remote_copy(
                src_ref=send_c.at[c, to], dst_ref=out.at[me_s, :, pl.ds(c * step, step)],
                send_sem=c_send, recv_sem=c_recv, device_id=(to, me_r), device_id_type=MESH,
            ).start()
        out[me_s, :, pl.ds(c * step, step)] = send_c[c, me_s]

    waits(got_a.at[:, pl.ds(0, rows - 1)], a_send, a_send).wait_send()
    waits(got_b.at[:, pl.ds(0, shares - 1)], b_send, b_send).wait_send()
    waits(send_c.at[:, pl.ds(0, shares - 1)], c_send, c_send).wait_send()
    waits(out.at[pl.ds(0, shares - 1)], c_send, c_recv).wait_recv()


def solution(mesh):
    shares, rows = mesh.shape["share"], mesh.shape["row"]
    table = constants()

    def body(remaining_coded_pieces, alive_piece_indices, slab_starting_positions):
        block, columns = remaining_coded_pieces.shape[1:]
        step = block // CHUNKS
        f32 = jnp.float32
        tiled = remaining_coded_pieces.reshape(block // SUBLANES, SUBLANES, columns // LANES, LANES).transpose(0, 2, 1, 3)
        dma = pltpu.SemaphoreType.DMA
        decoded = pl.pallas_call(
            functools.partial(kernel, shares, rows, CHUNKS),
            out_shape=jax.ShapeDtypeStruct((shares, 2, block, LANES), f32),
            in_specs=[
                pl.BlockSpec(memory_space=pltpu.SMEM),
                pl.BlockSpec(memory_space=pltpu.SMEM),
                pl.BlockSpec(memory_space=pl.ANY),
                pl.BlockSpec(memory_space=pl.ANY),
            ],
            out_specs=pl.BlockSpec(memory_space=pltpu.VMEM),
            scratch_shapes=[
                pltpu.VMEM((block // SUBLANES, columns // LANES, SUBLANES, LANES), f32),
                pltpu.VMEM((24, LANES), f32),
                pltpu.VMEM((K, LANES), f32),
                pltpu.VMEM((K, K, LANES), f32),
                pltpu.VMEM((CHUNKS, rows, step, LANES), f32),
                pltpu.VMEM((CHUNKS, rows, step, LANES), f32),
                pltpu.VMEM((CHUNKS, shares, 2, step, LANES), f32),
                pltpu.VMEM((CHUNKS, shares, 2, step, LANES), f32),
                dma((2,)),
                dma,
                dma((CHUNKS,)),
                dma,
                dma((CHUNKS,)),
                dma,
                dma,
            ],
            compiler_params=pltpu.CompilerParams(collective_id=0, has_side_effects=True),
            name="decode",
        )(alive_piece_indices, slab_starting_positions, tiled, jnp.asarray(table))
        return decoded.reshape(1, shares * 2 * block, LANES)

    return jax.shard_map(
        body, mesh=mesh, in_specs=(P("share", "row", None), P(), P()), out_specs=P("share", None, "row"), check_vma=False
    )
```

```python
import functools

import jax
import jax.numpy as jnp
import numpy as np
from jax import lax
from jax.experimental import pallas as pl
from jax.experimental.pallas import tpu as pltpu
from jax.sharding import PartitionSpec as P

K = 16
CODED_PIECES_ALL = 20
W = 2048
LANES = 128
SUBLANES = 8
MESH = pl.DeviceIdType.MESH


def constants():
    table = np.zeros((24, LANES), np.float32)
    theta = np.pi * (2.0 * np.arange(K) + 1.0) / (2.0 * K)
    degrees = np.arange(K)[:, None]
    scale = np.where(degrees == 0, 1.0, 2.0) / K
    table[:K, :K] = scale * np.cos(degrees * theta[None, :])
    table[K, :K] = np.cos(theta)
    numbers = np.arange(CODED_PIECES_ALL)
    table[K + 1, :CODED_PIECES_ALL] = np.cos(np.pi * (2.0 * numbers + 1.0) / (2.0 * CODED_PIECES_ALL))
    return table


def weights_into(table, alive, points_ref, w_ref):
    rows = lax.broadcasted_iota(jnp.int32, (K, LANES), 0)
    lanes = lax.broadcasted_iota(jnp.int32, (K, LANES), 1)
    number = jnp.zeros((K, LANES), jnp.int32)
    for i in range(K):
        number = jnp.where(rows == i, alive[i], number)
    nodes = jnp.broadcast_to(table[K + 1 : K + 2, :], (K, LANES))
    points = jnp.sum(jnp.where(lanes == number, nodes, 0.0), axis=1, keepdims=True)
    points = jnp.broadcast_to(points, (K, LANES))
    points_ref[...] = points
    samples = table[K : K + 1, :]
    over = jnp.ones((K, LANES), jnp.float32)
    under = jnp.ones((K, LANES), jnp.float32)
    for j in range(K):
        point = points_ref[j : j + 1, :]
        over = over * jnp.where(rows == j, 1.0, samples - point)
        under = under * jnp.where(rows == j, 1.0, points - point)
    lagrange = over / under
    for k in range(K):
        total = jnp.sum(lagrange * table[k : k + 1, :], axis=1, keepdims=True)
        w_ref[k] = jnp.broadcast_to(total, (K, LANES))


def each_in_half(me, count, half, act, unless=None):
    size = count // 2
    mine = me // size

    def run():
        @pl.when(mine != half)
        def _():
            act(half * size + lax.rem(me, size))

        for d in range(1, size):
            act(half * size + lax.rem(me + d, size))

    if unless is None:
        run()
    else:
        pl.when(unless == 0)(run)


def kernel(
    shares, rows,
    alive_hbm, starts_hbm, x_hbm, table_hbm, out,
    alive, starts, x, table, points, w, send_a, got_a, got_b, send_c,
    load_sems, a_send, a_recv, b_send, b_recv, c_send, c_recv, late_row, late_share,
):
    me_s = lax.axis_index("share")
    me_r = lax.axis_index("row")
    half_r, half_s = rows // 2, shares // 2
    late_r, late_s = me_r // half_r, me_s // half_s

    barrier = pltpu.get_barrier_semaphore()

    def greet_row(to):
        pl.semaphore_signal(barrier, inc=1, device_id=(me_s, to), device_id_type=MESH)

    def greet_share(to):
        pl.semaphore_signal(barrier, inc=1, device_id=(to, me_r), device_id_type=MESH)

    each_in_half(me_r, rows, 1, greet_row)
    each_in_half(me_s, shares, 1, greet_share)
    each_in_half(me_r, rows, 0, greet_row, unless=late_r)
    each_in_half(me_s, shares, 0, greet_share, unless=late_s)

    load_x = pltpu.make_async_copy(x_hbm, x, load_sems.at[0])
    load_starts = pltpu.make_async_copy(starts_hbm, starts, load_sems.at[1])
    load_alive = pltpu.make_async_copy(alive_hbm, alive, load_sems.at[2])
    load_table = pltpu.make_async_copy(table_hbm, table, load_sems.at[3])
    load_starts.start()
    load_x.start()
    load_alive.start()
    load_table.start()

    load_starts.wait()
    load_x.wait()
    for h in range(2):
        first = starts[h]
        for b in range(W // LANES):
            for t in range(x.shape[0]):
                send_a[h * (W // LANES) + b, t * SUBLANES : (t + 1) * SUBLANES] = x[t, first + b]

    pl.semaphore_wait(barrier, half_r - 1 + half_s - 1 + half_r * late_r + half_s * late_s)

    def announce_row(to):
        pl.semaphore_signal(late_row, inc=1, device_id=(me_s, to), device_id_type=MESH)

    def announce_share(to):
        pl.semaphore_signal(late_share, inc=1, device_id=(to, me_r), device_id_type=MESH)

    @pl.when(late_r == 1)
    def _():
        each_in_half(me_r, rows, 0, announce_row)

    @pl.when(late_s == 1)
    def _():
        each_in_half(me_s, shares, 0, announce_share)

    def spread_row(to):
        pltpu.make_async_remote_copy(
            src_ref=send_a.at[to], dst_ref=got_a.at[me_r],
            send_sem=a_send, recv_sem=a_recv.at[late_r], device_id=(me_s, to), device_id_type=MESH,
        ).start()

    each_in_half(me_r, rows, 0, spread_row)
    got_a[me_r] = send_a[me_r]

    @pl.when(late_r == 0)
    def _():
        pl.semaphore_wait(late_row, half_r)

    each_in_half(me_r, rows, 1, spread_row)

    load_alive.wait()
    load_table.wait()
    weights_into(table, alive, points, w)

    def waits(ref, send, recv):
        return pltpu.make_async_remote_copy(
            src_ref=ref, dst_ref=ref, send_sem=send, recv_sem=recv, device_id=(me_s, me_r), device_id_type=MESH
        )

    for c in range(2):

        @pl.when(late_r == c)
        def _():
            waits(got_a.at[pl.ds(0, half_r - 1)], a_send, a_recv.at[c]).wait_recv()

        @pl.when(late_r != c)
        def _():
            waits(got_a.at[pl.ds(0, half_r)], a_send, a_recv.at[c]).wait_recv()

        def spread_share(to):
            pltpu.make_async_remote_copy(
                src_ref=got_a.at[c * half_r + to], dst_ref=got_b.at[c, me_s],
                send_sem=b_send, recv_sem=b_recv.at[c], device_id=(to, me_r), device_id_type=MESH,
            ).start()

        each_in_half(me_s, shares, 0, spread_share)
        got_b[c, me_s] = got_a[c * half_r + me_s]
        if c == 0:

            @pl.when(late_s == 0)
            def _():
                pl.semaphore_wait(late_share, half_s)

        each_in_half(me_s, shares, 1, spread_share)

    for c in range(2):
        waits(got_b.at[c, pl.ds(0, shares - 1)], b_send, b_recv.at[c]).wait_recv()
        data = [got_b[c, i] for i in range(K)]
        for k in range(K):
            total = w[k, 0:1, :] * data[0]
            for i in range(1, K):
                total = total + w[k, i : i + 1, :] * data[i]
            send_c[c, k] = total

        def give_back(to):
            pltpu.make_async_remote_copy(
                src_ref=send_c.at[c, to], dst_ref=out.at[c * half_r + me_s],
                send_sem=c_send, recv_sem=c_recv, device_id=(to, me_r), device_id_type=MESH,
            ).start()

        each_in_half(me_s, shares, 0, give_back)
        each_in_half(me_s, shares, 1, give_back)
        out[c * half_r + me_s] = send_c[c, me_s]

    waits(got_a.at[pl.ds(0, rows - 1)], a_send, a_send).wait_send()
    waits(got_b.at[:, pl.ds(0, shares - 1)], b_send, b_send).wait_send()
    waits(send_c.at[:, pl.ds(0, shares - 1)], c_send, c_send).wait_send()
    waits(out.at[pl.ds(0, rows - 2)], c_send, c_recv).wait_recv()


def solution(mesh):
    shares, rows = mesh.shape["share"], mesh.shape["row"]
    table = constants()

    def body(remaining_coded_pieces, alive_piece_indices, slab_starting_positions):
        block, columns = remaining_coded_pieces.shape[1:]
        f32 = jnp.float32
        dma = pltpu.SemaphoreType.DMA
        tiled = remaining_coded_pieces.reshape(block // SUBLANES, SUBLANES, columns // LANES, LANES).transpose(0, 2, 1, 3)
        decoded = pl.pallas_call(
            functools.partial(kernel, shares, rows),
            out_shape=pltpu.VMEM((rows, block, LANES), f32),
            in_specs=[pl.BlockSpec(memory_space=pl.ANY)] * 4,
            out_specs=pl.BlockSpec(memory_space=pltpu.VMEM),
            scratch_shapes=[
                pltpu.SMEM((K,), jnp.int32),
                pltpu.SMEM((2,), jnp.int32),
                pltpu.VMEM((block // SUBLANES, columns // LANES, SUBLANES, LANES), f32),
                pltpu.VMEM((24, LANES), f32),
                pltpu.VMEM((K, LANES), f32),
                pltpu.VMEM((K, K, LANES), f32),
                pltpu.VMEM((rows, block, LANES), f32),
                pltpu.VMEM((rows, block, LANES), f32),
                pltpu.VMEM((2, shares, block, LANES), f32),
                pltpu.VMEM((2, shares, block, LANES), f32),
                dma((4,)),
                dma,
                dma((2,)),
                dma,
                dma((2,)),
                dma,
                dma,
                pltpu.SemaphoreType.REGULAR,
                pltpu.SemaphoreType.REGULAR,
            ],
            compiler_params=pltpu.CompilerParams(collective_id=0, has_side_effects=True),
            name="decode",
        )(alive_piece_indices, slab_starting_positions, tiled, jnp.asarray(table))
        return decoded.reshape(1, rows * block, LANES)

    return jax.shard_map(
        body, mesh=mesh, in_specs=(P("share", "row", None), P(), P()), out_specs=P("share", None, "row"), check_vma=False
    )
```

```python
import jax
import jax.numpy as jnp
import numpy as np
from jax import lax
from jax.experimental import pallas as pl
from jax.experimental.pallas import tpu as pltpu
from jax.sharding import PartitionSpec as P

K = 16
CODED_PIECES_ALL = 20
W = 2048
LANES = 128
SUBLANES = 8
CHUNKS = 4
CHUNK_ORDER = (0, 1, 2, 3)
X, Y, Z, CORES = 4, 8, 8, 2
MESH = pl.DeviceIdType.MESH


def constants():
    table = np.zeros((24, LANES), np.float32)
    theta = np.pi * (2.0 * np.arange(K) + 1.0) / (2.0 * K)
    degrees = np.arange(K)[:, None]
    scale = np.where(degrees == 0, 1.0, 2.0) / K
    table[:K, :K] = scale * np.cos(degrees * theta[None, :])
    table[K, :K] = np.cos(theta)
    numbers = np.arange(CODED_PIECES_ALL)
    table[K + 1, :CODED_PIECES_ALL] = np.cos(np.pi * (2.0 * numbers + 1.0) / (2.0 * CODED_PIECES_ALL))
    return table


def weights_into(table, alive, points_ref, w_ref):
    rows = lax.broadcasted_iota(jnp.int32, (K, LANES), 0)
    lanes = lax.broadcasted_iota(jnp.int32, (K, LANES), 1)
    number = jnp.zeros((K, LANES), jnp.int32)
    for i in range(K):
        number = jnp.where(rows == i, alive[i], number)
    nodes = jnp.broadcast_to(table[K + 1 : K + 2, :], (K, LANES))
    points = jnp.sum(jnp.where(lanes == number, nodes, 0.0), axis=1, keepdims=True)
    points = jnp.broadcast_to(points, (K, LANES))
    points_ref[...] = points
    samples = table[K : K + 1, :]
    over = jnp.ones((K, LANES), jnp.float32)
    under = jnp.ones((K, LANES), jnp.float32)
    for j in range(K):
        point = points_ref[j : j + 1, :]
        over = over * jnp.where(rows == j, 1.0, samples - point)
        under = under * jnp.where(rows == j, 1.0, points - point)
    lagrange = over / under
    for k in range(K):
        total = jnp.sum(lagrange * table[k : k + 1, :], axis=1, keepdims=True)
        w_ref[k] = jnp.broadcast_to(total, (K, LANES))


def far_first(sizes):
    offsets = [(a, b) for a in range(sizes[0]) for b in range(sizes[1])]
    return sorted(offsets, key=lambda o: (-sum(min(d, n - d) for d, n in zip(o, sizes)), o))


SHARE_ORDER = far_first((Z, CORES))
HALF_Y = Y // 2


def each_in_half(me, size, half, act):
    @pl.when(me // size != half)
    def _():
        act(half * size + lax.rem(me, size))

    for d in range(1, size):
        act(half * size + lax.rem(me + d, size))


def kernel(
    alive_hbm, starts_hbm, x_hbm, table_hbm, out,
    alive, starts, x, table, points, w, send_a, got_a, got_b, send_c,
    load_sems, a_send, a_recv, b_send, b_recv, c_send, c_recv, below_sems, above_sems,
):
    shares, rows = Z * CORES, Y * X
    half_r, half_s = rows // 2, shares // 2
    sources = rows // CHUNKS
    step = got_b.shape[2]
    parts = got_a.shape[1] // step
    me_s = lax.axis_index("share")
    me_r = lax.axis_index("row")
    my_y, my_x = me_r // X, lax.rem(me_r, X)
    my_z, my_core = me_s // CORES, lax.rem(me_s, CORES)
    late = me_r // half_r
    place = lax.rem(my_y, HALF_Y)

    def share_at(dz, dc):
        return lax.rem(my_z + dz, Z) * CORES + lax.rem(my_core + dc, CORES)

    def tell(semaphore, share, row):
        pl.semaphore_signal(semaphore, inc=1, device_id=(share, row), device_id_type=MESH)

    barrier = pltpu.get_barrier_semaphore()

    load_x = pltpu.make_async_copy(x_hbm, x, load_sems.at[0])
    load_starts = pltpu.make_async_copy(starts_hbm, starts, load_sems.at[1])
    load_alive = pltpu.make_async_copy(alive_hbm, alive, load_sems.at[2])
    load_table = pltpu.make_async_copy(table_hbm, table, load_sems.at[3])
    load_starts.start()
    load_x.start()

    each_in_half(me_r, half_r, 0, lambda to: tell(barrier, me_s, to))

    @pl.when(late == 0)
    def _():
        each_in_half(me_r, half_r, 1, lambda to: tell(barrier, me_s, to))

    @pl.when(late == 1)
    def _():
        for dx in (2, 1, 3):
            tell(barrier, me_s, my_y * X + lax.rem(my_x + dx, X))

        @pl.when(place > 0)
        def _():
            tell(barrier, me_s, me_r - X)

        @pl.when(place < HALF_Y - 1)
        def _():
            tell(barrier, me_s, me_r + X)

    for offset in SHARE_ORDER[:-1]:
        tell(barrier, share_at(*offset), me_r)

    load_alive.start()
    load_table.start()
    load_starts.wait()
    load_x.wait()
    for h in range(2):
        first = starts[h]
        for b in range(W // LANES):
            for t in range(x.shape[0]):
                send_a[h * (W // LANES) + b, t * SUBLANES : (t + 1) * SUBLANES] = x[t, first + b]

    neighbours = 1 + lax.rem((place + 1) // 2, 2)
    pl.semaphore_wait(barrier, shares - 1 + (1 - late) * (rows - 1) + late * (half_r + X - 1 + neighbours))

    def spread_row(to):
        pltpu.make_async_remote_copy(
            src_ref=send_a.at[to], dst_ref=got_a.at[me_r],
            send_sem=a_send, recv_sem=a_recv.at[me_r // sources], device_id=(me_s, to), device_id_type=MESH,
        ).start()

    def spread_group(y):
        for dx in (2, 1, 3, 0):
            spread_row(y * X + lax.rem(my_x + dx, X))

    @pl.when(late == 0)
    def _():
        each_in_half(me_r, half_r, 0, spread_row)
        each_in_half(me_r, half_r, 1, spread_row)

    @pl.when(late == 1)
    def _():
        @pl.when(place > 0)
        def _():
            tell(above_sems.at[0], me_s, me_r - X)

        @pl.when(place < HALF_Y - 1)
        def _():
            tell(below_sems.at[0], me_s, me_r + X)

        each_in_half(me_r, half_r, 0, spread_row)
        for dx in (2, 1, 3):
            spread_row(my_y * X + lax.rem(my_x + dx, X))
        for j in range(1, HALF_Y):

            @pl.when(place >= j)
            def _():
                pl.semaphore_wait(below_sems.at[j - 1], 1)
                if j < HALF_Y - 1:

                    @pl.when(place < HALF_Y - 1)
                    def _():
                        tell(below_sems.at[j], me_s, me_r + X)

            @pl.when(place + j < HALF_Y)
            def _():
                pl.semaphore_wait(above_sems.at[j - 1], 1)
                if j < HALF_Y - 1:

                    @pl.when(place > 0)
                    def _():
                        tell(above_sems.at[j], me_s, me_r - X)

            @pl.when(place >= j)
            def _():
                spread_group(my_y - j)

            @pl.when(place + j < HALF_Y)
            def _():
                spread_group(my_y + j)

    got_a[me_r] = send_a[me_r]

    load_alive.wait()
    load_table.wait()
    weights_into(table, alive, points, w)

    def waits(ref, send, recv):
        return pltpu.make_async_remote_copy(
            src_ref=ref, dst_ref=ref, send_sem=send, recv_sem=recv, device_id=(me_s, me_r), device_id_type=MESH
        )

    def piece(c, owner):
        return c * sources + owner // parts, pl.ds(lax.rem(owner, parts) * step, step)

    for c in CHUNK_ORDER:

        @pl.when(me_r // sources == c)
        def _():
            waits(got_a.at[pl.ds(0, sources - 1)], a_send, a_recv.at[c]).wait_recv()

        @pl.when(me_r // sources != c)
        def _():
            waits(got_a.at[pl.ds(0, sources)], a_send, a_recv.at[c]).wait_recv()

        for offset in SHARE_ORDER[:-1]:
            to = share_at(*offset)
            pltpu.make_async_remote_copy(
                src_ref=got_a.at[*piece(c, to)], dst_ref=got_b.at[c, me_s],
                send_sem=b_send, recv_sem=b_recv.at[c], device_id=(to, me_r), device_id_type=MESH,
            ).start()
        got_b[c, me_s] = got_a[*piece(c, me_s)]

    for c in CHUNK_ORDER:
        waits(got_b.at[c, pl.ds(0, shares - 1)], b_send, b_recv.at[c]).wait_recv()
        for t in range(step // SUBLANES):
            part = slice(t * SUBLANES, (t + 1) * SUBLANES)
            data = [got_b[c, i, part] for i in range(K)]
            for k in range(K):
                total = w[k, 0:1, :] * data[0]
                for i in range(1, K):
                    total = total + w[k, i : i + 1, :] * data[i]
                send_c[c, k, part] = total

        def give_back(to):
            pltpu.make_async_remote_copy(
                src_ref=send_c.at[c, to], dst_ref=out.at[*piece(c, me_s)],
                send_sem=c_send, recv_sem=c_recv, device_id=(to, me_r), device_id_type=MESH,
            ).start()

        each_in_half(me_s, half_s, 0, give_back)
        each_in_half(me_s, half_s, 1, give_back)
        out[*piece(c, me_s)] = send_c[c, me_s]

    waits(got_a.at[pl.ds(0, rows - 1)], a_send, a_send).wait_send()
    waits(got_b.at[:, pl.ds(0, shares - 1)], b_send, b_send).wait_send()
    waits(send_c.at[:, pl.ds(0, shares - 1)], c_send, c_send).wait_send()
    waits(send_c.at[:, pl.ds(0, shares - 1)], c_send, c_recv).wait_recv()


def solution(mesh):
    shares, rows = mesh.shape["share"], mesh.shape["row"]
    table = constants()

    def body(remaining_coded_pieces, alive_piece_indices, slab_starting_positions):
        block, columns = remaining_coded_pieces.shape[1:]
        f32 = jnp.float32
        dma = pltpu.SemaphoreType.DMA
        tiled = remaining_coded_pieces.reshape(block // SUBLANES, SUBLANES, columns // LANES, LANES).transpose(0, 2, 1, 3)
        decoded = pl.pallas_call(
            kernel,
            out_shape=pltpu.VMEM((rows, block, LANES), f32),
            in_specs=[pl.BlockSpec(memory_space=pl.ANY)] * 4,
            out_specs=pl.BlockSpec(memory_space=pltpu.VMEM),
            scratch_shapes=[
                pltpu.SMEM((K,), jnp.int32),
                pltpu.SMEM((2,), jnp.int32),
                pltpu.VMEM((block // SUBLANES, columns // LANES, SUBLANES, LANES), f32),
                pltpu.VMEM((24, LANES), f32),
                pltpu.VMEM((K, LANES), f32),
                pltpu.VMEM((K, K, LANES), f32),
                pltpu.VMEM((rows, block, LANES), f32),
                pltpu.VMEM((rows, block, LANES), f32),
                pltpu.VMEM((CHUNKS, shares, 2 * block // CHUNKS, LANES), f32),
                pltpu.VMEM((CHUNKS, shares, 2 * block // CHUNKS, LANES), f32),
                dma((4,)),
                dma,
                dma((CHUNKS,)),
                dma,
                dma((CHUNKS,)),
                dma,
                dma,
                pltpu.SemaphoreType.REGULAR((HALF_Y - 1,)),
                pltpu.SemaphoreType.REGULAR((HALF_Y - 1,)),
            ],
            compiler_params=pltpu.CompilerParams(collective_id=0, has_side_effects=True),
            name="decode",
        )(alive_piece_indices, slab_starting_positions, tiled, jnp.asarray(table))
        return decoded.reshape(1, rows * block, LANES)

    return jax.shard_map(
        body, mesh=mesh, in_specs=(P("share", "row", None), P(), P()), out_specs=P("share", None, "row"), check_vma=False
    )
```

```python
import jax
import jax.numpy as jnp
import numpy as np
from jax import lax
from jax.experimental import pallas as pl
from jax.experimental.pallas import tpu as pltpu
from jax.sharding import PartitionSpec as P

K = 16
CODED_PIECES_ALL = 20
W = 2048
LANES = 128
SUBLANES = 8
CHUNKS = 4
X, Y, Z, CORES = 4, 8, 8, 2
MESH = pl.DeviceIdType.MESH


def constants():
    table = np.zeros((24, LANES), np.float32)
    theta = np.pi * (2.0 * np.arange(K) + 1.0) / (2.0 * K)
    degrees = np.arange(K)[:, None]
    scale = np.where(degrees == 0, 1.0, 2.0) / K
    table[:K, :K] = scale * np.cos(degrees * theta[None, :])
    table[K, :K] = np.cos(theta)
    numbers = np.arange(CODED_PIECES_ALL)
    table[K + 1, :CODED_PIECES_ALL] = np.cos(np.pi * (2.0 * numbers + 1.0) / (2.0 * CODED_PIECES_ALL))
    return table


def weights_into(table, alive, points_ref, w_ref):
    rows = lax.broadcasted_iota(jnp.int32, (K, LANES), 0)
    lanes = lax.broadcasted_iota(jnp.int32, (K, LANES), 1)
    number = jnp.zeros((K, LANES), jnp.int32)
    for i in range(K):
        number = jnp.where(rows == i, alive[i], number)
    nodes = jnp.broadcast_to(table[K + 1 : K + 2, :], (K, LANES))
    points = jnp.sum(jnp.where(lanes == number, nodes, 0.0), axis=1, keepdims=True)
    points = jnp.broadcast_to(points, (K, LANES))
    points_ref[...] = points
    samples = table[K : K + 1, :]
    over = jnp.ones((K, LANES), jnp.float32)
    under = jnp.ones((K, LANES), jnp.float32)
    for j in range(K):
        point = points_ref[j : j + 1, :]
        over = over * jnp.where(rows == j, 1.0, samples - point)
        under = under * jnp.where(rows == j, 1.0, points - point)
    lagrange = over / under
    for k in range(K):
        total = jnp.sum(lagrange * table[k : k + 1, :], axis=1, keepdims=True)
        w_ref[k] = jnp.broadcast_to(total, (K, LANES))


def far_first(sizes):
    offsets = [(a, b) for a in range(sizes[0]) for b in range(sizes[1])]
    return sorted(offsets, key=lambda o: (-sum(min(d, n - d) for d, n in zip(o, sizes)), o))


SHARE_ORDER = far_first((Z, CORES))
HALF_Y = Y // 2


def each_in_half(me, size, half, act):
    @pl.when(me // size != half)
    def _():
        act(half * size + lax.rem(me, size))

    for d in range(1, size):
        act(half * size + lax.rem(me + d, size))


def kernel(
    alive_hbm, starts_hbm, x_hbm, table_hbm, out,
    alive, starts, x, table, points, w, send_a, got_a, got_b, send_c,
    load_sems, a_send, a_recv, b_send, b_recv, c_send, c_recv, below_sems, above_sems, late_share,
):
    shares, rows = Z * CORES, Y * X
    half_r, half_s = rows // 2, shares // 2
    sources = rows // CHUNKS
    step = got_b.shape[2]
    parts = got_a.shape[1] // step
    me_s = lax.axis_index("share")
    me_r = lax.axis_index("row")
    my_y, my_x = me_r // X, lax.rem(me_r, X)
    my_z, my_core = me_s // CORES, lax.rem(me_s, CORES)
    late = me_r // half_r
    place = lax.rem(my_y, HALF_Y)

    def share_at(dz, dc):
        return lax.rem(my_z + dz, Z) * CORES + lax.rem(my_core + dc, CORES)

    def tell(semaphore, share, row):
        pl.semaphore_signal(semaphore, inc=1, device_id=(share, row), device_id_type=MESH)

    barrier = pltpu.get_barrier_semaphore()

    load_x = pltpu.make_async_copy(x_hbm, x, load_sems.at[0])
    load_starts = pltpu.make_async_copy(starts_hbm, starts, load_sems.at[1])
    load_alive = pltpu.make_async_copy(alive_hbm, alive, load_sems.at[2])
    load_table = pltpu.make_async_copy(table_hbm, table, load_sems.at[3])
    load_starts.start()
    load_x.start()

    @pl.when(late == 0)
    def _():
        each_in_half(me_r, half_r, 1, lambda to: tell(barrier, me_s, to))
        each_in_half(me_r, half_r, 0, lambda to: tell(barrier, me_s, to))

    @pl.when(late == 1)
    def _():
        for dx in (2, 1, 3):
            tell(barrier, me_s, my_y * X + lax.rem(my_x + dx, X))

        @pl.when(place > 0)
        def _():
            tell(barrier, me_s, me_r - X)

        @pl.when(place < HALF_Y - 1)
        def _():
            tell(barrier, me_s, me_r + X)

    late_s = me_s // half_s
    each_in_half(me_s, half_s, 1, lambda to: tell(barrier, to, me_r))

    @pl.when(late_s == 0)
    def _():
        each_in_half(me_s, half_s, 0, lambda to: tell(barrier, to, me_r))


    load_alive.start()
    load_table.start()
    load_starts.wait()
    load_x.wait()
    for h in range(2):
        first = starts[h]
        for b in range(W // LANES):
            for t in range(x.shape[0]):
                send_a[h * (W // LANES) + b, t * SUBLANES : (t + 1) * SUBLANES] = x[t, first + b]

    neighbours = 1 + lax.rem((place + 1) // 2, 2)
    pl.semaphore_wait(barrier, half_s - 1 + half_s * late_s + half_r - 1 + late * (X + neighbours))

    @pl.when(late_s == 1)
    def _():
        each_in_half(me_s, half_s, 0, lambda to: tell(late_share, to, me_r))

    def spread_row(to):
        pltpu.make_async_remote_copy(
            src_ref=send_a.at[to], dst_ref=got_a.at[me_r],
            send_sem=a_send, recv_sem=a_recv.at[me_r // sources], device_id=(me_s, to), device_id_type=MESH,
        ).start()

    def spread_group(y):
        for dx in (2, 1, 3, 0):
            spread_row(y * X + lax.rem(my_x + dx, X))

    @pl.when(late == 0)
    def _():
        each_in_half(me_r, half_r, 0, spread_row)

        def from_below():
            for j in range(2):
                pl.semaphore_wait(below_sems.at[j], 1)

                @pl.when(place < HALF_Y - 1)
                def _():
                    tell(below_sems.at[j], me_s, me_r + X)

                spread_group(Y - 1 - j)

        def from_above():
            for j in range(2):
                pl.semaphore_wait(above_sems.at[j], 1)

                @pl.when(place > 0)
                def _():
                    tell(above_sems.at[j], me_s, me_r - X)

                spread_group(HALF_Y + j)

        pl.when(place < 2)(from_below)
        from_above()
        pl.when(place >= 2)(from_below)

    @pl.when(late == 1)
    def _():
        above, below = lax.rem(me_r + X, rows), me_r - X
        tell(below_sems.at[0], me_s, above)
        tell(above_sems.at[0], me_s, below)
        each_in_half(me_r, half_r, 0, spread_row)
        for dx in (2, 1, 3):
            spread_row(my_y * X + lax.rem(my_x + dx, X))
        for j in range(1, HALF_Y):

            @pl.when(place >= j)
            def _():
                pl.semaphore_wait(below_sems.at[j - 1], 1)
                if j == 1:
                    tell(below_sems.at[1], me_s, above)
                if j == 2:

                    @pl.when(place < HALF_Y - 1)
                    def _():
                        tell(below_sems.at[2], me_s, above)

            @pl.when(place + j < HALF_Y)
            def _():
                pl.semaphore_wait(above_sems.at[j - 1], 1)
                if j == 1:
                    tell(above_sems.at[1], me_s, below)
                if j == 2:

                    @pl.when(place > 0)
                    def _():
                        tell(above_sems.at[2], me_s, below)

            @pl.when(place >= j)
            def _():
                spread_group(my_y - j)

            @pl.when(place + j < HALF_Y)
            def _():
                spread_group(my_y + j)

    got_a[me_r] = send_a[me_r]

    load_alive.wait()
    load_table.wait()
    weights_into(table, alive, points, w)

    def waits(ref, send, recv):
        return pltpu.make_async_remote_copy(
            src_ref=ref, dst_ref=ref, send_sem=send, recv_sem=recv, device_id=(me_s, me_r), device_id_type=MESH
        )

    def piece(c, owner):
        return c * sources + owner // parts, pl.ds(lax.rem(owner, parts) * step, step)

    for n in range(CHUNKS):
        c = lax.rem(n + CHUNKS // 2 * late, CHUNKS)

        @pl.when(me_r // sources == c)
        def _():
            waits(got_a.at[pl.ds(0, sources - 1)], a_send, a_recv.at[c]).wait_recv()

        @pl.when(me_r // sources != c)
        def _():
            waits(got_a.at[pl.ds(0, sources)], a_send, a_recv.at[c]).wait_recv()

        def spread_share(to):
            pltpu.make_async_remote_copy(
                src_ref=got_a.at[*piece(c, to)], dst_ref=got_b.at[c, me_s],
                send_sem=b_send, recv_sem=b_recv.at[c], device_id=(to, me_r), device_id_type=MESH,
            ).start()

        each_in_half(me_s, half_s, 0, spread_share)
        if n == 0:

            @pl.when(late_s == 0)
            def _():
                pl.semaphore_wait(late_share, half_s)

        each_in_half(me_s, half_s, 1, spread_share)
        got_b[c, me_s] = got_a[*piece(c, me_s)]

    for n in range(CHUNKS):
        c = lax.rem(n + CHUNKS // 2 * late, CHUNKS)
        waits(got_b.at[c, pl.ds(0, shares - 1)], b_send, b_recv.at[c]).wait_recv()
        for t in range(step // SUBLANES):
            part = slice(t * SUBLANES, (t + 1) * SUBLANES)
            data = [got_b[c, i, part] for i in range(K)]
            for k in range(K):
                total = w[k, 0:1, :] * data[0]
                for i in range(1, K):
                    total = total + w[k, i : i + 1, :] * data[i]
                send_c[c, k, part] = total

        def give_back(to):
            pltpu.make_async_remote_copy(
                src_ref=send_c.at[c, to], dst_ref=out.at[*piece(c, me_s)],
                send_sem=c_send, recv_sem=c_recv, device_id=(to, me_r), device_id_type=MESH,
            ).start()

        each_in_half(me_s, half_s, 0, give_back)
        each_in_half(me_s, half_s, 1, give_back)
        out[*piece(c, me_s)] = send_c[c, me_s]

    waits(got_a.at[pl.ds(0, rows - 1)], a_send, a_send).wait_send()
    waits(got_b.at[:, pl.ds(0, shares - 1)], b_send, b_send).wait_send()
    waits(send_c.at[:, pl.ds(0, shares - 1)], c_send, c_send).wait_send()
    waits(send_c.at[:, pl.ds(0, shares - 1)], c_send, c_recv).wait_recv()


def solution(mesh):
    shares, rows = mesh.shape["share"], mesh.shape["row"]
    table = constants()

    def body(remaining_coded_pieces, alive_piece_indices, slab_starting_positions):
        block, columns = remaining_coded_pieces.shape[1:]
        f32 = jnp.float32
        dma = pltpu.SemaphoreType.DMA
        tiled = remaining_coded_pieces.reshape(block // SUBLANES, SUBLANES, columns // LANES, LANES).transpose(0, 2, 1, 3)
        decoded = pl.pallas_call(
            kernel,
            out_shape=pltpu.VMEM((rows, block, LANES), f32),
            in_specs=[pl.BlockSpec(memory_space=pl.ANY)] * 4,
            out_specs=pl.BlockSpec(memory_space=pltpu.VMEM),
            scratch_shapes=[
                pltpu.SMEM((K,), jnp.int32),
                pltpu.SMEM((2,), jnp.int32),
                pltpu.VMEM((block // SUBLANES, columns // LANES, SUBLANES, LANES), f32),
                pltpu.VMEM((24, LANES), f32),
                pltpu.VMEM((K, LANES), f32),
                pltpu.VMEM((K, K, LANES), f32),
                pltpu.VMEM((rows, block, LANES), f32),
                pltpu.VMEM((rows, block, LANES), f32),
                pltpu.VMEM((CHUNKS, shares, 2 * block // CHUNKS, LANES), f32),
                pltpu.VMEM((CHUNKS, shares, 2 * block // CHUNKS, LANES), f32),
                dma((4,)),
                dma,
                dma((CHUNKS,)),
                dma,
                dma((CHUNKS,)),
                dma,
                dma,
                pltpu.SemaphoreType.REGULAR((HALF_Y - 1,)),
                pltpu.SemaphoreType.REGULAR((HALF_Y - 1,)),
                pltpu.SemaphoreType.REGULAR,
            ],
            compiler_params=pltpu.CompilerParams(collective_id=0, has_side_effects=True),
            name="decode",
        )(alive_piece_indices, slab_starting_positions, tiled, jnp.asarray(table))
        return decoded.reshape(1, rows * block, LANES)

    return jax.shard_map(
        body, mesh=mesh, in_specs=(P("share", "row", None), P(), P()), out_specs=P("share", None, "row"), check_vma=False
    )
```

```python
import jax
import jax.numpy as jnp
import numpy as np
from jax import lax
from jax.experimental import pallas as pl
from jax.experimental.pallas import tpu as pltpu
from jax.sharding import PartitionSpec as P

K = 16
CODED_PIECES_ALL = 20
W = 2048
LANES = 128
SUBLANES = 8
CHUNKS = 4
X, Y, Z, CORES = 4, 8, 8, 2
MESH = pl.DeviceIdType.MESH


def constants():
    table = np.zeros((24, LANES), np.float32)
    theta = np.pi * (2.0 * np.arange(K) + 1.0) / (2.0 * K)
    degrees = np.arange(K)[:, None]
    scale = np.where(degrees == 0, 1.0, 2.0) / K
    table[:K, :K] = scale * np.cos(degrees * theta[None, :])
    table[K, :K] = np.cos(theta)
    numbers = np.arange(CODED_PIECES_ALL)
    table[K + 1, :CODED_PIECES_ALL] = np.cos(np.pi * (2.0 * numbers + 1.0) / (2.0 * CODED_PIECES_ALL))
    return table


def weights_into(table, alive, points_ref, w_ref):
    rows = lax.broadcasted_iota(jnp.int32, (K, LANES), 0)
    lanes = lax.broadcasted_iota(jnp.int32, (K, LANES), 1)
    number = jnp.zeros((K, LANES), jnp.int32)
    for i in range(K):
        number = jnp.where(rows == i, alive[i], number)
    nodes = jnp.broadcast_to(table[K + 1 : K + 2, :], (K, LANES))
    points = jnp.sum(jnp.where(lanes == number, nodes, 0.0), axis=1, keepdims=True)
    points = jnp.broadcast_to(points, (K, LANES))
    points_ref[...] = points
    samples = table[K : K + 1, :]
    over = jnp.ones((K, LANES), jnp.float32)
    under = jnp.ones((K, LANES), jnp.float32)
    for j in range(K):
        point = points_ref[j : j + 1, :]
        over = over * jnp.where(rows == j, 1.0, samples - point)
        under = under * jnp.where(rows == j, 1.0, points - point)
    lagrange = over / under
    for k in range(K):
        total = jnp.sum(lagrange * table[k : k + 1, :], axis=1, keepdims=True)
        w_ref[k] = jnp.broadcast_to(total, (K, LANES))


def far_first(sizes):
    offsets = [(a, b) for a in range(sizes[0]) for b in range(sizes[1])]
    return sorted(offsets, key=lambda o: (-sum(min(d, n - d) for d, n in zip(o, sizes)), o))


SHARE_ORDER = far_first((Z, CORES))
HALF_Y = Y // 2
LOW = (3, 2, 0, 1)
HIGH = (0, 1, 2, 3)


def each_in_half(me, size, half, act):
    @pl.when(me // size != half)
    def _():
        act(half * size + lax.rem(me, size))

    for d in range(1, size):
        act(half * size + lax.rem(me + d, size))


def kernel(
    alive_hbm, starts_hbm, x_hbm, table_hbm, out,
    alive, starts, x, table, points, w, send_a, got_a, got_b, send_c,
    load_sems, a_send, a_recv, b_send, b_recv, c_send, c_recv, below_sems, above_sems, late_share, group_sems,
):
    shares, rows = Z * CORES, Y * X
    half_r, half_s = rows // 2, shares // 2
    sources = rows // CHUNKS
    step = got_b.shape[2]
    parts = got_a.shape[1] // step
    me_s = lax.axis_index("share")
    me_r = lax.axis_index("row")
    my_y, my_x = me_r // X, lax.rem(me_r, X)
    my_z, my_core = me_s // CORES, lax.rem(me_s, CORES)
    late = me_r // half_r
    place = lax.rem(my_y, HALF_Y)

    def share_at(dz, dc):
        return lax.rem(my_z + dz, Z) * CORES + lax.rem(my_core + dc, CORES)

    def tell(semaphore, share, row):
        pl.semaphore_signal(semaphore, inc=1, device_id=(share, row), device_id_type=MESH)

    barrier = pltpu.get_barrier_semaphore()

    load_x = pltpu.make_async_copy(x_hbm, x, load_sems.at[0])
    load_starts = pltpu.make_async_copy(starts_hbm, starts, load_sems.at[1])
    load_alive = pltpu.make_async_copy(alive_hbm, alive, load_sems.at[2])
    load_table = pltpu.make_async_copy(table_hbm, table, load_sems.at[3])
    load_starts.start()
    load_x.start()

    @pl.when(late == 0)
    def _():
        each_in_half(me_r, half_r, 1, lambda to: tell(barrier, me_s, to))
        each_in_half(me_r, half_r, 0, lambda to: tell(barrier, me_s, to))

    @pl.when(late == 1)
    def _():
        for dx in (2, 1, 3):
            tell(barrier, me_s, my_y * X + lax.rem(my_x + dx, X))

        @pl.when(place > 0)
        def _():
            tell(barrier, me_s, me_r - X)

        @pl.when(place < HALF_Y - 1)
        def _():
            tell(barrier, me_s, me_r + X)

    late_s = me_s // half_s
    each_in_half(me_s, half_s, 1, lambda to: tell(barrier, to, me_r))

    @pl.when(late_s == 0)
    def _():
        each_in_half(me_s, half_s, 0, lambda to: tell(barrier, to, me_r))


    load_alive.start()
    load_table.start()
    load_starts.wait()
    load_x.wait()
    for h in range(2):
        first = starts[h]
        for b in range(W // LANES):
            for t in range(x.shape[0]):
                send_a[h * (W // LANES) + b, t * SUBLANES : (t + 1) * SUBLANES] = x[t, first + b]

    neighbours = 1 + lax.rem((place + 1) // 2, 2)
    pl.semaphore_wait(barrier, half_s - 1 + half_s * late_s + half_r - 1 + late * (X + neighbours))

    @pl.when(late_s == 1)
    def _():
        each_in_half(me_s, half_s, 0, lambda to: tell(late_share, to, me_r))

    def spread_row(to):
        pltpu.make_async_remote_copy(
            src_ref=send_a.at[to], dst_ref=got_a.at[me_r],
            send_sem=a_send, recv_sem=a_recv.at[me_r // sources], device_id=(me_s, to), device_id_type=MESH,
        ).start()

    def spread_group(y):
        for dx in (2, 1, 3, 0):
            spread_row(y * X + lax.rem(my_x + dx, X))

    @pl.when(late == 0)
    def _():
        each_in_half(me_r, half_r, 0, spread_row)

        for n in range(HALF_Y):
            group = jnp.where(place < 2, LOW[n], HIGH[n])
            pl.semaphore_wait(group_sems.at[group], 1)
            spread_group(HALF_Y + group)

    @pl.when(late == 1)
    def _():
        above, below = lax.rem(me_r + X, rows), me_r - X
        for early in range(HALF_Y):
            tell(group_sems.at[place], me_s, early * X + my_x)

        @pl.when(place < HALF_Y - 1)
        def _():
            tell(below_sems.at[0], me_s, above)

        @pl.when(place > 0)
        def _():
            tell(above_sems.at[0], me_s, below)

        each_in_half(me_r, half_r, 0, spread_row)
        for dx in (2, 1, 3):
            spread_row(my_y * X + lax.rem(my_x + dx, X))
        for j in range(1, HALF_Y):

            @pl.when(place >= j)
            def _():
                pl.semaphore_wait(below_sems.at[j - 1], 1)
                if j < HALF_Y - 1:

                    @pl.when(place < HALF_Y - 1)
                    def _():
                        tell(below_sems.at[j], me_s, above)

            @pl.when(place + j < HALF_Y)
            def _():
                pl.semaphore_wait(above_sems.at[j - 1], 1)
                if j < HALF_Y - 1:

                    @pl.when(place > 0)
                    def _():
                        tell(above_sems.at[j], me_s, below)

            @pl.when(place >= j)
            def _():
                spread_group(my_y - j)

            @pl.when(place + j < HALF_Y)
            def _():
                spread_group(my_y + j)

    got_a[me_r] = send_a[me_r]

    load_alive.wait()
    load_table.wait()
    weights_into(table, alive, points, w)

    def waits(ref, send, recv):
        return pltpu.make_async_remote_copy(
            src_ref=ref, dst_ref=ref, send_sem=send, recv_sem=recv, device_id=(me_s, me_r), device_id_type=MESH
        )

    def piece(c, owner):
        return c * sources + owner // parts, pl.ds(lax.rem(owner, parts) * step, step)

    pair = me_r // sources
    across = CHUNKS - 1 - pair

    def chunk_at(n):
        near = pair if n < 2 else across
        return near if n % 2 == 0 else near + 1 - 2 * lax.rem(near, 2)

    for n in range(CHUNKS):
        c = chunk_at(n)

        @pl.when(me_r // sources == c)
        def _():
            waits(got_a.at[pl.ds(0, sources - 1)], a_send, a_recv.at[c]).wait_recv()

        @pl.when(me_r // sources != c)
        def _():
            waits(got_a.at[pl.ds(0, sources)], a_send, a_recv.at[c]).wait_recv()

        def spread_share(to):
            pltpu.make_async_remote_copy(
                src_ref=got_a.at[*piece(c, to)], dst_ref=got_b.at[c, me_s],
                send_sem=b_send, recv_sem=b_recv.at[c], device_id=(to, me_r), device_id_type=MESH,
            ).start()

        each_in_half(me_s, half_s, 0, spread_share)
        if n == 0:

            @pl.when(late_s == 0)
            def _():
                pl.semaphore_wait(late_share, half_s)

        each_in_half(me_s, half_s, 1, spread_share)
        got_b[c, me_s] = got_a[*piece(c, me_s)]

    for n in range(CHUNKS):
        c = chunk_at(n)
        waits(got_b.at[c, pl.ds(0, shares - 1)], b_send, b_recv.at[c]).wait_recv()
        for t in range(step // SUBLANES):
            part = slice(t * SUBLANES, (t + 1) * SUBLANES)
            data = [got_b[c, i, part] for i in range(K)]
            for k in range(K):
                total = w[k, 0:1, :] * data[0]
                for i in range(1, K):
                    total = total + w[k, i : i + 1, :] * data[i]
                send_c[c, k, part] = total

        def give_back(to):
            pltpu.make_async_remote_copy(
                src_ref=send_c.at[c, to], dst_ref=out.at[*piece(c, me_s)],
                send_sem=c_send, recv_sem=c_recv, device_id=(to, me_r), device_id_type=MESH,
            ).start()

        each_in_half(me_s, half_s, 0, give_back)
        each_in_half(me_s, half_s, 1, give_back)
        out[*piece(c, me_s)] = send_c[c, me_s]

    waits(got_a.at[pl.ds(0, rows - 1)], a_send, a_send).wait_send()
    waits(got_b.at[:, pl.ds(0, shares - 1)], b_send, b_send).wait_send()
    waits(send_c.at[:, pl.ds(0, shares - 1)], c_send, c_send).wait_send()
    waits(send_c.at[:, pl.ds(0, shares - 1)], c_send, c_recv).wait_recv()


def solution(mesh):
    shares, rows = mesh.shape["share"], mesh.shape["row"]
    table = constants()

    def body(remaining_coded_pieces, alive_piece_indices, slab_starting_positions):
        block, columns = remaining_coded_pieces.shape[1:]
        f32 = jnp.float32
        dma = pltpu.SemaphoreType.DMA
        tiled = remaining_coded_pieces.reshape(block // SUBLANES, SUBLANES, columns // LANES, LANES).transpose(0, 2, 1, 3)
        decoded = pl.pallas_call(
            kernel,
            out_shape=pltpu.VMEM((rows, block, LANES), f32),
            in_specs=[pl.BlockSpec(memory_space=pl.ANY)] * 4,
            out_specs=pl.BlockSpec(memory_space=pltpu.VMEM),
            scratch_shapes=[
                pltpu.SMEM((K,), jnp.int32),
                pltpu.SMEM((2,), jnp.int32),
                pltpu.VMEM((block // SUBLANES, columns // LANES, SUBLANES, LANES), f32),
                pltpu.VMEM((24, LANES), f32),
                pltpu.VMEM((K, LANES), f32),
                pltpu.VMEM((K, K, LANES), f32),
                pltpu.VMEM((rows, block, LANES), f32),
                pltpu.VMEM((rows, block, LANES), f32),
                pltpu.VMEM((CHUNKS, shares, 2 * block // CHUNKS, LANES), f32),
                pltpu.VMEM((CHUNKS, shares, 2 * block // CHUNKS, LANES), f32),
                dma((4,)),
                dma,
                dma((CHUNKS,)),
                dma,
                dma((CHUNKS,)),
                dma,
                dma,
                pltpu.SemaphoreType.REGULAR((HALF_Y - 1,)),
                pltpu.SemaphoreType.REGULAR((HALF_Y - 1,)),
                pltpu.SemaphoreType.REGULAR,
                pltpu.SemaphoreType.REGULAR((HALF_Y,)),
            ],
            compiler_params=pltpu.CompilerParams(collective_id=0, has_side_effects=True),
            name="decode",
        )(alive_piece_indices, slab_starting_positions, tiled, jnp.asarray(table))
        return decoded.reshape(1, rows * block, LANES)

    return jax.shard_map(
        body, mesh=mesh, in_specs=(P("share", "row", None), P(), P()), out_specs=P("share", None, "row"), check_vma=False
    )
```

```python
import jax
import jax.numpy as jnp
import numpy as np
from jax import lax
from jax.experimental import pallas as pl
from jax.experimental.pallas import tpu as pltpu
from jax.sharding import PartitionSpec as P

K = 16
CODED_PIECES_ALL = 20
W = 2048
LANES = 128
SUBLANES = 8
CHUNKS = 4
X, Y, Z, CORES = 4, 8, 8, 2
MESH = pl.DeviceIdType.MESH


def constants():
    table = np.zeros((24, LANES), np.float32)
    theta = np.pi * (2.0 * np.arange(K) + 1.0) / (2.0 * K)
    degrees = np.arange(K)[:, None]
    scale = np.where(degrees == 0, 1.0, 2.0) / K
    table[:K, :K] = scale * np.cos(degrees * theta[None, :])
    table[K, :K] = np.cos(theta)
    numbers = np.arange(CODED_PIECES_ALL)
    table[K + 1, :CODED_PIECES_ALL] = np.cos(np.pi * (2.0 * numbers + 1.0) / (2.0 * CODED_PIECES_ALL))
    return table


def weights_into(table, alive, points_ref, w_ref):
    rows = lax.broadcasted_iota(jnp.int32, (K, LANES), 0)
    lanes = lax.broadcasted_iota(jnp.int32, (K, LANES), 1)
    number = jnp.zeros((K, LANES), jnp.int32)
    for i in range(K):
        number = jnp.where(rows == i, alive[i], number)
    nodes = jnp.broadcast_to(table[K + 1 : K + 2, :], (K, LANES))
    points = jnp.sum(jnp.where(lanes == number, nodes, 0.0), axis=1, keepdims=True)
    points = jnp.broadcast_to(points, (K, LANES))
    points_ref[...] = points
    samples = table[K : K + 1, :]
    over = jnp.ones((K, LANES), jnp.float32)
    under = jnp.ones((K, LANES), jnp.float32)
    for j in range(K):
        point = points_ref[j : j + 1, :]
        over = over * jnp.where(rows == j, 1.0, samples - point)
        under = under * jnp.where(rows == j, 1.0, points - point)
    lagrange = over / under
    for k in range(K):
        total = jnp.sum(lagrange * table[k : k + 1, :], axis=1, keepdims=True)
        w_ref[k] = jnp.broadcast_to(total, (K, LANES))


def far_first(sizes):
    offsets = [(a, b) for a in range(sizes[0]) for b in range(sizes[1])]
    return sorted(offsets, key=lambda o: (-sum(min(d, n - d) for d, n in zip(o, sizes)), o))


SHARE_ORDER = far_first((Z, CORES))
HALF_Y = Y // 2
LOW = (3, 2, 0, 1)
HIGH = (0, 1, 2, 3)


def each_in_half(me, size, half, act):
    @pl.when(me // size != half)
    def _():
        act(half * size + lax.rem(me, size))

    for d in range(1, size):
        act(half * size + lax.rem(me + d, size))


def kernel(
    alive_hbm, starts_hbm, x_hbm, table_hbm, out,
    alive, starts, x, table, points, w, send_a, got_a, got_b, send_c,
    load_sems, a_send, a_recv, b_send, b_recv, c_send, c_recv, below_sems, above_sems, late_share, group_sems,
):
    shares, rows = Z * CORES, Y * X
    half_r, half_s = rows // 2, shares // 2
    sources = rows // CHUNKS
    step = got_b.shape[2]
    parts = got_a.shape[1] // step
    me_s = lax.axis_index("share")
    me_r = lax.axis_index("row")
    my_y, my_x = me_r // X, lax.rem(me_r, X)
    my_z, my_core = me_s // CORES, lax.rem(me_s, CORES)
    late = me_r // half_r
    place = lax.rem(my_y, HALF_Y)

    def share_at(dz, dc):
        return lax.rem(my_z + dz, Z) * CORES + lax.rem(my_core + dc, CORES)

    def tell(semaphore, share, row):
        pl.semaphore_signal(semaphore, inc=1, device_id=(share, row), device_id_type=MESH)

    barrier = pltpu.get_barrier_semaphore()

    load_x = pltpu.make_async_copy(x_hbm, x, load_sems.at[0])
    load_starts = pltpu.make_async_copy(starts_hbm, starts, load_sems.at[1])
    load_alive = pltpu.make_async_copy(alive_hbm, alive, load_sems.at[2])
    load_table = pltpu.make_async_copy(table_hbm, table, load_sems.at[3])
    load_starts.start()
    load_x.start()

    @pl.when(late == 0)
    def _():
        each_in_half(me_r, half_r, 1, lambda to: tell(barrier, me_s, to))
        each_in_half(me_r, half_r, 0, lambda to: tell(barrier, me_s, to))

    @pl.when(late == 1)
    def _():
        for dx in (2, 1, 3):
            tell(barrier, me_s, my_y * X + lax.rem(my_x + dx, X))

        @pl.when(place > 0)
        def _():
            tell(barrier, me_s, me_r - X)

        @pl.when(place < HALF_Y - 1)
        def _():
            tell(barrier, me_s, me_r + X)

    late_s = me_s // half_s
    each_in_half(me_s, half_s, 1, lambda to: tell(barrier, to, me_r))

    @pl.when(late_s == 0)
    def _():
        each_in_half(me_s, half_s, 0, lambda to: tell(barrier, to, me_r))


    load_alive.start()
    load_table.start()
    load_starts.wait()
    load_x.wait()
    for h in range(2):
        first = starts[h]
        for b in range(W // LANES):
            for t in range(x.shape[0]):
                send_a[h * (W // LANES) + b, t * SUBLANES : (t + 1) * SUBLANES] = x[t, first + b]

    neighbours = 1 + lax.rem((place + 1) // 2, 2)
    pl.semaphore_wait(barrier, half_s - 1 + half_s * late_s + half_r - 1 + late * (X + neighbours))

    @pl.when(late_s == 1)
    def _():
        each_in_half(me_s, half_s, 0, lambda to: tell(late_share, to, me_r))

    def spread_row(to):
        pltpu.make_async_remote_copy(
            src_ref=send_a.at[to], dst_ref=got_a.at[me_r],
            send_sem=a_send, recv_sem=a_recv.at[me_r // sources], device_id=(me_s, to), device_id_type=MESH,
        ).start()

    def spread_group(y):
        for dx in (2, 1, 3, 0):
            spread_row(y * X + lax.rem(my_x + dx, X))

    @pl.when(late == 0)
    def _():
        each_in_half(me_r, half_r, 0, spread_row)

        for n in range(HALF_Y):
            group = jnp.where(place < 2, LOW[n], HIGH[n])
            pl.semaphore_wait(group_sems.at[group], 1)
            spread_group(HALF_Y + group)

    @pl.when(late == 1)
    def _():
        above, below = lax.rem(me_r + X, rows), me_r - X
        for early in range(HALF_Y):
            tell(group_sems.at[place], me_s, early * X + my_x)

        @pl.when(place < HALF_Y - 1)
        def _():
            tell(below_sems.at[0], me_s, above)

        @pl.when(place > 0)
        def _():
            tell(above_sems.at[0], me_s, below)

        for y in (0, 1, 2, 3):
            spread_group(y)

        for dx in (2, 1, 3):
            spread_row(my_y * X + lax.rem(my_x + dx, X))
        for j in range(1, HALF_Y):

            @pl.when(place >= j)
            def _():
                pl.semaphore_wait(below_sems.at[j - 1], 1)
                if j < HALF_Y - 1:

                    @pl.when(place < HALF_Y - 1)
                    def _():
                        tell(below_sems.at[j], me_s, above)

            @pl.when(place + j < HALF_Y)
            def _():
                pl.semaphore_wait(above_sems.at[j - 1], 1)
                if j < HALF_Y - 1:

                    @pl.when(place > 0)
                    def _():
                        tell(above_sems.at[j], me_s, below)

            @pl.when(place >= j)
            def _():
                spread_group(my_y - j)

            @pl.when(place + j < HALF_Y)
            def _():
                spread_group(my_y + j)

    got_a[me_r] = send_a[me_r]

    load_alive.wait()
    load_table.wait()
    weights_into(table, alive, points, w)

    def waits(ref, send, recv):
        return pltpu.make_async_remote_copy(
            src_ref=ref, dst_ref=ref, send_sem=send, recv_sem=recv, device_id=(me_s, me_r), device_id_type=MESH
        )

    def piece(c, owner):
        return c * sources + owner // parts, pl.ds(lax.rem(owner, parts) * step, step)

    pair = me_r // sources
    across = CHUNKS - 1 - pair

    def chunk_at(n):
        near = pair if n < 2 else across
        return near if n % 2 == 0 else near + 1 - 2 * lax.rem(near, 2)

    for n in range(CHUNKS):
        c = chunk_at(n)

        @pl.when(me_r // sources == c)
        def _():
            waits(got_a.at[pl.ds(0, sources - 1)], a_send, a_recv.at[c]).wait_recv()

        @pl.when(me_r // sources != c)
        def _():
            waits(got_a.at[pl.ds(0, sources)], a_send, a_recv.at[c]).wait_recv()

        def spread_share(to):
            pltpu.make_async_remote_copy(
                src_ref=got_a.at[*piece(c, to)], dst_ref=got_b.at[c, me_s],
                send_sem=b_send, recv_sem=b_recv.at[c], device_id=(to, me_r), device_id_type=MESH,
            ).start()

        each_in_half(me_s, half_s, 0, spread_share)
        if n == 0:

            @pl.when(late_s == 0)
            def _():
                pl.semaphore_wait(late_share, half_s)

        each_in_half(me_s, half_s, 1, spread_share)
        got_b[c, me_s] = got_a[*piece(c, me_s)]

    for n in range(CHUNKS):
        c = chunk_at(n)
        waits(got_b.at[c, pl.ds(0, shares - 1)], b_send, b_recv.at[c]).wait_recv()
        for t in range(step // SUBLANES):
            part = slice(t * SUBLANES, (t + 1) * SUBLANES)
            data = [got_b[c, i, part] for i in range(K)]
            for k in range(K):
                total = w[k, 0:1, :] * data[0]
                for i in range(1, K):
                    total = total + w[k, i : i + 1, :] * data[i]
                send_c[c, k, part] = total

        def give_back(to):
            pltpu.make_async_remote_copy(
                src_ref=send_c.at[c, to], dst_ref=out.at[*piece(c, me_s)],
                send_sem=c_send, recv_sem=c_recv, device_id=(to, me_r), device_id_type=MESH,
            ).start()

        each_in_half(me_s, half_s, 0, give_back)
        each_in_half(me_s, half_s, 1, give_back)
        out[*piece(c, me_s)] = send_c[c, me_s]

    waits(got_a.at[pl.ds(0, rows - 1)], a_send, a_send).wait_send()
    waits(got_b.at[:, pl.ds(0, shares - 1)], b_send, b_send).wait_send()
    waits(send_c.at[:, pl.ds(0, shares - 1)], c_send, c_send).wait_send()
    waits(send_c.at[:, pl.ds(0, shares - 1)], c_send, c_recv).wait_recv()


def solution(mesh):
    shares, rows = mesh.shape["share"], mesh.shape["row"]
    table = constants()

    def body(remaining_coded_pieces, alive_piece_indices, slab_starting_positions):
        block, columns = remaining_coded_pieces.shape[1:]
        f32 = jnp.float32
        dma = pltpu.SemaphoreType.DMA
        tiled = remaining_coded_pieces.reshape(block // SUBLANES, SUBLANES, columns // LANES, LANES).transpose(0, 2, 1, 3)
        decoded = pl.pallas_call(
            kernel,
            out_shape=pltpu.VMEM((rows, block, LANES), f32),
            in_specs=[pl.BlockSpec(memory_space=pl.ANY)] * 4,
            out_specs=pl.BlockSpec(memory_space=pltpu.VMEM),
            scratch_shapes=[
                pltpu.SMEM((K,), jnp.int32),
                pltpu.SMEM((2,), jnp.int32),
                pltpu.VMEM((block // SUBLANES, columns // LANES, SUBLANES, LANES), f32),
                pltpu.VMEM((24, LANES), f32),
                pltpu.VMEM((K, LANES), f32),
                pltpu.VMEM((K, K, LANES), f32),
                pltpu.VMEM((rows, block, LANES), f32),
                pltpu.VMEM((rows, block, LANES), f32),
                pltpu.VMEM((CHUNKS, shares, 2 * block // CHUNKS, LANES), f32),
                pltpu.VMEM((CHUNKS, shares, 2 * block // CHUNKS, LANES), f32),
                dma((4,)),
                dma,
                dma((CHUNKS,)),
                dma,
                dma((CHUNKS,)),
                dma,
                dma,
                pltpu.SemaphoreType.REGULAR((HALF_Y - 1,)),
                pltpu.SemaphoreType.REGULAR((HALF_Y - 1,)),
                pltpu.SemaphoreType.REGULAR,
                pltpu.SemaphoreType.REGULAR((HALF_Y,)),
            ],
            compiler_params=pltpu.CompilerParams(collective_id=0, has_side_effects=True),
            name="decode",
        )(alive_piece_indices, slab_starting_positions, tiled, jnp.asarray(table))
        return decoded.reshape(1, rows * block, LANES)

    return jax.shard_map(
        body, mesh=mesh, in_specs=(P("share", "row", None), P(), P()), out_specs=P("share", None, "row"), check_vma=False
    )
```

```python
import jax
import jax.numpy as jnp
import numpy as np
from jax import lax
from jax.experimental import pallas as pl
from jax.experimental.pallas import tpu as pltpu
from jax.sharding import PartitionSpec as P

K = 16
CODED_PIECES_ALL = 20
W = 2048
LANES = 128
SUBLANES = 8
CHUNKS = 4
X, Y, Z, CORES = 4, 8, 8, 2
MESH = pl.DeviceIdType.MESH


def constants():
    table = np.zeros((24, LANES), np.float32)
    theta = np.pi * (2.0 * np.arange(K) + 1.0) / (2.0 * K)
    degrees = np.arange(K)[:, None]
    scale = np.where(degrees == 0, 1.0, 2.0) / K
    table[:K, :K] = scale * np.cos(degrees * theta[None, :])
    table[K, :K] = np.cos(theta)
    numbers = np.arange(CODED_PIECES_ALL)
    table[K + 1, :CODED_PIECES_ALL] = np.cos(np.pi * (2.0 * numbers + 1.0) / (2.0 * CODED_PIECES_ALL))
    return table


def weights_into(table, alive, points_ref, w_ref):
    rows = lax.broadcasted_iota(jnp.int32, (K, LANES), 0)
    lanes = lax.broadcasted_iota(jnp.int32, (K, LANES), 1)
    number = jnp.zeros((K, LANES), jnp.int32)
    for i in range(K):
        number = jnp.where(rows == i, alive[i], number)
    nodes = jnp.broadcast_to(table[K + 1 : K + 2, :], (K, LANES))
    points = jnp.sum(jnp.where(lanes == number, nodes, 0.0), axis=1, keepdims=True)
    points = jnp.broadcast_to(points, (K, LANES))
    points_ref[...] = points
    samples = table[K : K + 1, :]
    over = jnp.ones((K, LANES), jnp.float32)
    under = jnp.ones((K, LANES), jnp.float32)
    for j in range(K):
        point = points_ref[j : j + 1, :]
        over = over * jnp.where(rows == j, 1.0, samples - point)
        under = under * jnp.where(rows == j, 1.0, points - point)
    lagrange = over / under
    for k in range(K):
        total = jnp.sum(lagrange * table[k : k + 1, :], axis=1, keepdims=True)
        w_ref[k] = jnp.broadcast_to(total, (K, LANES))


def far_first(sizes):
    offsets = [(a, b) for a in range(sizes[0]) for b in range(sizes[1])]
    return sorted(offsets, key=lambda o: (-sum(min(d, n - d) for d, n in zip(o, sizes)), o))


SHARE_ORDER = far_first((Z, CORES))
HALF_Y = Y // 2
LOW = (3, 2, 0, 1)
HIGH = (0, 1, 2, 3)


def each_in_half(me, size, half, act):
    @pl.when(me // size != half)
    def _():
        act(half * size + lax.rem(me, size))

    for d in range(1, size):
        act(half * size + lax.rem(me + d, size))


def kernel(
    alive_hbm, starts_hbm, x_hbm, table_hbm, out,
    alive, starts, x, table, points, w, send_a, got_a, got_b, send_c,
    load_sems, a_send, a_recv, b_send, b_recv, c_send, c_recv, below_sems, above_sems, late_share, group_sems,
):
    shares, rows = Z * CORES, Y * X
    half_r, half_s = rows // 2, shares // 2
    sources = rows // CHUNKS
    step = got_b.shape[2]
    parts = got_a.shape[1] // step
    me_s = lax.axis_index("share")
    me_r = lax.axis_index("row")
    my_y, my_x = me_r // X, lax.rem(me_r, X)
    my_z, my_core = me_s // CORES, lax.rem(me_s, CORES)
    late = me_r // half_r
    place = lax.rem(my_y, HALF_Y)

    def share_at(dz, dc):
        return lax.rem(my_z + dz, Z) * CORES + lax.rem(my_core + dc, CORES)

    def tell(semaphore, share, row):
        pl.semaphore_signal(semaphore, inc=1, device_id=(share, row), device_id_type=MESH)

    barrier = pltpu.get_barrier_semaphore()

    load_x = pltpu.make_async_copy(x_hbm, x, load_sems.at[0])
    load_starts = pltpu.make_async_copy(starts_hbm, starts, load_sems.at[1])
    load_alive = pltpu.make_async_copy(alive_hbm, alive, load_sems.at[2])
    load_table = pltpu.make_async_copy(table_hbm, table, load_sems.at[3])
    load_starts.start()
    load_x.start()

    @pl.when(late == 0)
    def _():
        each_in_half(me_r, half_r, 1, lambda to: tell(barrier, me_s, to))
        each_in_half(me_r, half_r, 0, lambda to: tell(barrier, me_s, to))

    @pl.when(late == 1)
    def _():
        for dx in (2, 1, 3):
            tell(barrier, me_s, my_y * X + lax.rem(my_x + dx, X))

        @pl.when(place > 0)
        def _():
            tell(barrier, me_s, me_r - X)

        @pl.when(place < HALF_Y - 1)
        def _():
            tell(barrier, me_s, me_r + X)

    late_s = me_s // half_s
    each_in_half(me_s, half_s, 1, lambda to: tell(barrier, to, me_r))

    @pl.when(late_s == 0)
    def _():
        each_in_half(me_s, half_s, 0, lambda to: tell(barrier, to, me_r))


    load_alive.start()
    load_table.start()
    load_starts.wait()
    load_x.wait()
    for h in range(2):
        first = starts[h]
        for b in range(W // LANES):
            for t in range(x.shape[0]):
                send_a[h * (W // LANES) + b, t * SUBLANES : (t + 1) * SUBLANES] = x[t, first + b]

    neighbours = 1 + lax.rem((place + 1) // 2, 2)
    pl.semaphore_wait(barrier, half_s - 1 + half_s * late_s + half_r - 1 + late * (X + neighbours))

    @pl.when(late_s == 1)
    def _():
        each_in_half(me_s, half_s, 0, lambda to: tell(late_share, to, me_r))

    def spread_row(to):
        pltpu.make_async_remote_copy(
            src_ref=send_a.at[to], dst_ref=got_a.at[me_r],
            send_sem=a_send, recv_sem=a_recv.at[me_r // sources], device_id=(me_s, to), device_id_type=MESH,
        ).start()

    def spread_group(y):
        for column in range(X):
            spread_row(y * X + column)

    @pl.when(late == 0)
    def _():
        each_in_half(me_r, half_r, 0, spread_row)

        for n in range(HALF_Y):
            group = jnp.where(place < 2, LOW[n], HIGH[n])
            pl.semaphore_wait(group_sems.at[group], 1)
            spread_group(HALF_Y + group)

    @pl.when(late == 1)
    def _():
        above, below = lax.rem(me_r + X, rows), me_r - X
        for early in range(HALF_Y):
            tell(group_sems.at[place], me_s, early * X + my_x)

        @pl.when(place < HALF_Y - 1)
        def _():
            tell(below_sems.at[0], me_s, above)

        @pl.when(place > 0)
        def _():
            tell(above_sems.at[0], me_s, below)

        for y in (0, 1, 2, 3):
            spread_group(y)

        for dx in (2, 1, 3):
            spread_row(my_y * X + lax.rem(my_x + dx, X))
        for j in range(1, HALF_Y):

            @pl.when(place >= j)
            def _():
                pl.semaphore_wait(below_sems.at[j - 1], 1)
                if j < HALF_Y - 1:

                    @pl.when(place < HALF_Y - 1)
                    def _():
                        tell(below_sems.at[j], me_s, above)

            @pl.when(place + j < HALF_Y)
            def _():
                pl.semaphore_wait(above_sems.at[j - 1], 1)
                if j < HALF_Y - 1:

                    @pl.when(place > 0)
                    def _():
                        tell(above_sems.at[j], me_s, below)

            @pl.when(place >= j)
            def _():
                spread_group(my_y - j)

            @pl.when(place + j < HALF_Y)
            def _():
                spread_group(my_y + j)

    got_a[me_r] = send_a[me_r]

    load_alive.wait()
    load_table.wait()
    weights_into(table, alive, points, w)

    def waits(ref, send, recv):
        return pltpu.make_async_remote_copy(
            src_ref=ref, dst_ref=ref, send_sem=send, recv_sem=recv, device_id=(me_s, me_r), device_id_type=MESH
        )

    def piece(c, owner):
        return c * sources + owner // parts, pl.ds(lax.rem(owner, parts) * step, step)

    pair = me_r // sources
    across = CHUNKS - 1 - pair

    def chunk_at(n):
        near = pair if n < 2 else across
        return near if n % 2 == 0 else near + 1 - 2 * lax.rem(near, 2)

    for n in range(CHUNKS):
        c = chunk_at(n)

        @pl.when(me_r // sources == c)
        def _():
            waits(got_a.at[pl.ds(0, sources - 1)], a_send, a_recv.at[c]).wait_recv()

        @pl.when(me_r // sources != c)
        def _():
            waits(got_a.at[pl.ds(0, sources)], a_send, a_recv.at[c]).wait_recv()

        def spread_share(to):
            pltpu.make_async_remote_copy(
                src_ref=got_a.at[*piece(c, to)], dst_ref=got_b.at[c, me_s],
                send_sem=b_send, recv_sem=b_recv.at[c], device_id=(to, me_r), device_id_type=MESH,
            ).start()

        each_in_half(me_s, half_s, 0, spread_share)
        if n == 0:

            @pl.when(late_s == 0)
            def _():
                pl.semaphore_wait(late_share, half_s)

        each_in_half(me_s, half_s, 1, spread_share)
        got_b[c, me_s] = got_a[*piece(c, me_s)]

    for n in range(CHUNKS):
        c = chunk_at(n)
        waits(got_b.at[c, pl.ds(0, shares - 1)], b_send, b_recv.at[c]).wait_recv()
        for t in range(step // SUBLANES):
            part = slice(t * SUBLANES, (t + 1) * SUBLANES)
            data = [got_b[c, i, part] for i in range(K)]
            for k in range(K):
                total = w[k, 0:1, :] * data[0]
                for i in range(1, K):
                    total = total + w[k, i : i + 1, :] * data[i]
                send_c[c, k, part] = total

        def give_back(to):
            pltpu.make_async_remote_copy(
                src_ref=send_c.at[c, to], dst_ref=out.at[*piece(c, me_s)],
                send_sem=c_send, recv_sem=c_recv, device_id=(to, me_r), device_id_type=MESH,
            ).start()

        each_in_half(me_s, half_s, 0, give_back)
        each_in_half(me_s, half_s, 1, give_back)
        out[*piece(c, me_s)] = send_c[c, me_s]

    waits(got_a.at[pl.ds(0, rows - 1)], a_send, a_send).wait_send()
    waits(got_b.at[:, pl.ds(0, shares - 1)], b_send, b_send).wait_send()
    waits(send_c.at[:, pl.ds(0, shares - 1)], c_send, c_send).wait_send()
    waits(send_c.at[:, pl.ds(0, shares - 1)], c_send, c_recv).wait_recv()


def solution(mesh):
    shares, rows = mesh.shape["share"], mesh.shape["row"]
    table = constants()

    def body(remaining_coded_pieces, alive_piece_indices, slab_starting_positions):
        block, columns = remaining_coded_pieces.shape[1:]
        f32 = jnp.float32
        dma = pltpu.SemaphoreType.DMA
        tiled = remaining_coded_pieces.reshape(block // SUBLANES, SUBLANES, columns // LANES, LANES).transpose(0, 2, 1, 3)
        decoded = pl.pallas_call(
            kernel,
            out_shape=pltpu.VMEM((rows, block, LANES), f32),
            in_specs=[pl.BlockSpec(memory_space=pl.ANY)] * 4,
            out_specs=pl.BlockSpec(memory_space=pltpu.VMEM),
            scratch_shapes=[
                pltpu.SMEM((K,), jnp.int32),
                pltpu.SMEM((2,), jnp.int32),
                pltpu.VMEM((block // SUBLANES, columns // LANES, SUBLANES, LANES), f32),
                pltpu.VMEM((24, LANES), f32),
                pltpu.VMEM((K, LANES), f32),
                pltpu.VMEM((K, K, LANES), f32),
                pltpu.VMEM((rows, block, LANES), f32),
                pltpu.VMEM((rows, block, LANES), f32),
                pltpu.VMEM((CHUNKS, shares, 2 * block // CHUNKS, LANES), f32),
                pltpu.VMEM((CHUNKS, shares, 2 * block // CHUNKS, LANES), f32),
                dma((4,)),
                dma,
                dma((CHUNKS,)),
                dma,
                dma((CHUNKS,)),
                dma,
                dma,
                pltpu.SemaphoreType.REGULAR((HALF_Y - 1,)),
                pltpu.SemaphoreType.REGULAR((HALF_Y - 1,)),
                pltpu.SemaphoreType.REGULAR,
                pltpu.SemaphoreType.REGULAR((HALF_Y,)),
            ],
            compiler_params=pltpu.CompilerParams(collective_id=0, has_side_effects=True),
            name="decode",
        )(alive_piece_indices, slab_starting_positions, tiled, jnp.asarray(table))
        return decoded.reshape(1, rows * block, LANES)

    return jax.shard_map(
        body, mesh=mesh, in_specs=(P("share", "row", None), P(), P()), out_specs=P("share", None, "row"), check_vma=False
    )
```
